32 devices in a mesh: sec: 4 (over y, core), grp: 8 (over z, x).
Axes of the slice: x: 2, y: 2, z: 4, core: 2. Of those that a mesh axis runs over, the one named last changes fastest.
Arguments:
- positions: float32 [3, 16384], P(None, ('sec', 'grp')), may hold values from -9 to 9, as said below
- velocities: float32 [3, 16384], P(None, ('sec', 'grp')), may hold values from -4 to 4
- masses: float32 [16384], P(('sec', 'grp')), may hold values from 0.004 to 0.04
- near_list: int32 [64, 64], P(('sec', 'grp')), may hold values from 0 to 7, as said below
- near_count: int32 [64], P(('sec', 'grp')), may hold values from 1 to 64, as said below
- far_list: int32 [64, 32], P(('sec', 'grp')), may hold values from 0 to 63
Outputs:
- positions_out: float32 [3, 16384], P(None, ('sec', 'grp'))
- velocities_out: float32 [3, 16384], P(None, ('sec', 'grp'))
- accel_out: float32 [3, 16384], P(None, ('sec', 'grp'))
The draws below stay inside these ranges and needn't reach their ends.
Inputs may be any that keep to these rules, and one draw needn't show every extreme that they name: `positions`: within the range stated, particles of a block lie near one another and blocks of a group near their group. `near_list`: numbers within the group: the section index times 2 plus the block's place on its device. Slot 0 names the block itself. `near_count`: some block has all 64 slots used.
All inputs are finite; a program needn't handle non-finite values.
Results may differ from the reference program's by a relative error of at most 0.0001.
Values sent between devices are 32-bit elements; how exact they have to be, the bound alone decides.
A program may use at most 64 MiB of HBM per device.

```python
import math
import jax
import jax.numpy as jnp
from jax import lax

B = 256
NB_DEV = 2
LIST = 64
FAR = 32
GBLK = 8
NBLK = 64
NPART = 16384
N_GRP = 8


def draw_positions(key, part):
    first, second, third = jax.random.split(key, 3)
    groups = NBLK // GBLK
    centres = jax.random.uniform(first, (3, groups), jnp.float32, -4.0, 4.0)
    block_ids = jnp.arange(NBLK)
    group_of = block_ids // NB_DEV % groups
    block_centre = centres[:, group_of] + jax.random.uniform(second, (3, NBLK), jnp.float32, -1.5, 1.5)
    offsets = jnp.clip(0.6 * jax.random.normal(third, (3, NBLK, B), jnp.float32), -3.0, 3.0)
    return (block_centre[:, :, None] + offsets).reshape(3, NBLK * B)


def draw_near_list(key, part):
    groups = NBLK // GBLK
    block_ids = jnp.arange(NBLK, dtype=jnp.int32)
    section = block_ids // (NB_DEV * groups)
    own = section * NB_DEV + block_ids % NB_DEV
    listed = jax.random.randint(key, (NBLK, LIST), 0, GBLK, jnp.int32)
    return listed.at[:, 0].set(own)


def draw_near_count(key, part):
    first, second = jax.random.split(jax.random.fold_in(key, 7))
    devices = NBLK // NB_DEV
    level = jax.random.randint(first, (devices,), 0, 3, jnp.int32).at[0].set(0)
    most = LIST // jnp.left_shift(jnp.int32(1), level)
    block_ids = jnp.arange(NBLK, dtype=jnp.int32)
    device_of = block_ids // NB_DEV
    counts = jax.random.randint(second, (NBLK,), 1, most[device_of] + 1, jnp.int32)
    return jnp.where(block_ids % NB_DEV == 0, most[device_of], counts).astype(jnp.int32)


def plant(entries, key, smallest, high):
    longest = entries.shape.index(max(entries.shape))
    spots = []
    for shift in (0, 1):
        where = [jax.random.randint(jax.random.fold_in(key, axis), (), 0, length) for axis, length in enumerate(entries.shape)]
        where[longest] = (where[longest] + shift) % entries.shape[longest]
        spots.append(tuple(where))
    return entries.at[spots[0]].set(smallest).at[spots[1]].set(high)


def level_of(key, dims, pieces, low, top_value):
    gain, own = 1.0, jax.random.fold_in(key, 6)
    for position, shards_of in pieces:
        heights = jnp.exp(jax.random.uniform(jax.random.fold_in(own, position), (shards_of,), jnp.float32, low / len(pieces), top_value / len(pieces)))
        gain = gain * jnp.repeat(heights, dims[position] // shards_of).reshape([-1 if axis == position else 1 for axis in range(len(dims))])
    return gain


def centred(stream_key, shape, width, most, cuts=(), held_as=jnp.bfloat16):
    loudness = level_of(stream_key, shape, cuts, -0.22, 0.18) if cuts else 1.0
    values = jax.random.normal(stream_key, shape, jnp.float32) * width * loudness
    return jnp.minimum(jnp.maximum(values, -most), most).astype(held_as)


def setup_inputs(seed: int = 0) -> dict:
    keys = jax.random.split(jax.random.key(seed), 7)
    return {
        "positions": draw_positions(jax.random.fold_in(keys[6], 71), 0),
        "velocities": centred(keys[1], (3, NPART), 1.0, 4.0, ((1, 32),), jnp.float32),
        "masses": jnp.clip(jnp.exp(math.log(0.04) - 2.30258502 * jax.random.uniform(keys[2], (NPART,), jnp.float32) ** level_of(keys[2], (NPART,), ((0, 32),), -0.2, 0.2)), 0.004, 0.04),
        "near_list": draw_near_list(jax.random.fold_in(keys[6], 71), 0),
        "near_count": draw_near_count(jax.random.fold_in(keys[6], 71), 0),
        "far_list": plant(jax.random.randint(keys[5], (NBLK, FAR), 0, NBLK), jax.random.fold_in(keys[5], 1), 0, NBLK - 1).astype(jnp.int32),
    }


timestep = 0.05
softening = 0.25

def pair_accel(target, source):
    delta_x = source[0][:, None, :] - target[0][:, :, None]
    delta_y = source[1][:, None, :] - target[1][:, :, None]
    delta_z = source[2][:, None, :] - target[2][:, :, None]
    square = delta_x * delta_x + delta_y * delta_y + delta_z * delta_z + softening
    weight = source[3][:, None, :] / (square * jnp.sqrt(square))
    return jnp.stack([lax.optimization_barrier(jnp.sum(weight * delta_x, -1)), lax.optimization_barrier(jnp.sum(weight * delta_y, -1)), lax.optimization_barrier(jnp.sum(weight * delta_z, -1))])

def far_accel(target, moment):
    rel_x = target[0][:, None, :] - moment[1][:, :, None]
    rel_y = target[1][:, None, :] - moment[2][:, :, None]
    rel_z = target[2][:, None, :] - moment[3][:, :, None]
    square = rel_x * rel_x + rel_y * rel_y + rel_z * rel_z + softening
    inv_three = 1.0 / (square * jnp.sqrt(square))
    inv_five = inv_three / square
    inv_seven = inv_five / square
    quad_x = moment[4][..., None] * rel_x + moment[7][..., None] * rel_y + moment[8][..., None] * rel_z
    quad_y = moment[7][..., None] * rel_x + moment[5][..., None] * rel_y + moment[9][..., None] * rel_z
    quad_z = moment[8][..., None] * rel_x + moment[9][..., None] * rel_y + moment[6][..., None] * rel_z
    inner = rel_x * quad_x + rel_y * quad_y + rel_z * quad_z
    mass = moment[0][..., None]
    acc_x = lax.optimization_barrier(jnp.sum(-mass * rel_x * inv_three - quad_x * inv_five + 2.5 * inner * rel_x * inv_seven, 1))
    acc_y = lax.optimization_barrier(jnp.sum(-mass * rel_y * inv_three - quad_y * inv_five + 2.5 * inner * rel_y * inv_seven, 1))
    acc_z = lax.optimization_barrier(jnp.sum(-mass * rel_z * inv_three - quad_z * inv_five + 2.5 * inner * rel_z * inv_seven, 1))
    return jnp.stack([acc_x, acc_y, acc_z])

def block_moments(blocks):
    weight = blocks[3]
    mass = lax.optimization_barrier(jnp.sum(weight, -1))
    centre_x = lax.optimization_barrier(jnp.sum(weight * blocks[0], -1)) / mass
    centre_y = lax.optimization_barrier(jnp.sum(weight * blocks[1], -1)) / mass
    centre_z = lax.optimization_barrier(jnp.sum(weight * blocks[2], -1)) / mass
    off_x = blocks[0] - centre_x[:, None]
    off_y = blocks[1] - centre_y[:, None]
    off_z = blocks[2] - centre_z[:, None]
    radius = off_x * off_x + off_y * off_y + off_z * off_z
    return jnp.stack([mass, centre_x, centre_y, centre_z, lax.optimization_barrier(jnp.sum(weight * (3.0 * off_x * off_x - radius), -1)), lax.optimization_barrier(jnp.sum(weight * (3.0 * off_y * off_y - radius), -1)), lax.optimization_barrier(jnp.sum(weight * (3.0 * off_z * off_z - radius), -1)), lax.optimization_barrier(jnp.sum(3.0 * weight * off_x * off_y, -1)), lax.optimization_barrier(jnp.sum(3.0 * weight * off_x * off_z, -1)), lax.optimization_barrier(jnp.sum(3.0 * weight * off_y * off_z, -1))])

def accelerate(half, masses, global_near, near_count, far_list):
    blocks = jnp.concatenate([half, masses[None, :]], 0).reshape(4, NBLK, B)
    moments = block_moments(blocks)

    def one_block(index):
        target = blocks[:3, index][:, None, :]

        def add_slot(slot, total):
            source = blocks[:, global_near[index, slot]][:, None, :]
            return total + pair_accel(target, source)
        direct = lax.fori_loop(0, near_count[index], add_slot, jnp.zeros((3, 1, B), jnp.float32))
        far = far_accel(target, moments[:, far_list[index]][:, None, :])
        return (direct + far)[:, 0, :]
    result = lax.map(one_block, jnp.arange(NBLK, dtype=jnp.int32))
    return jnp.transpose(result, (1, 0, 2)).reshape(3, NBLK * B)

def reference(positions, velocities, masses, near_list, near_count, far_list):
    block_ids = jnp.arange(NBLK, dtype=jnp.int32)
    group_of = block_ids // NB_DEV % N_GRP
    section = near_list // NB_DEV
    place = near_list % NB_DEV
    global_near = ((section * N_GRP + group_of[:, None]) * NB_DEV + place).astype(jnp.int32)
    current = positions
    speed = velocities
    accel = jnp.zeros_like(positions)
    for step in range(2):
        half = current + 0.5 * timestep * speed
        accel = accelerate(half, masses, global_near, near_count, far_list)
        speed = speed + timestep * accel
        current = half + 0.5 * timestep * speed
    return (current, speed, accel)
```

```python
import functools

import jax
import jax.numpy as jnp
from jax import lax
from jax.experimental import pallas as pl
from jax.experimental.pallas import tpu as pltpu
from jax.sharding import PartitionSpec as P

timestep = 0.05
softening = 0.25
LANES = 128
ROWS = 8
MESH = pl.DeviceIdType.MESH


def peer(sec, r, n_sec):
    if n_sec % 2:
        return lax.rem(sec + r, n_sec)
    pair = lax.rem(sec // 2 + r // 2, n_sec // 2)
    return pair * 2 + lax.rem(sec + r, 2)


def own_moments(blocks):
    lane = lax.broadcasted_iota(jnp.int32, (1, LANES), 1)
    rows = []
    for x, y, z, m in blocks:
        total = lambda v: jnp.sum(v, axis=1, keepdims=True)
        mass = total(m)
        cx, cy, cz = total(m * x) / mass, total(m * y) / mass, total(m * z) / mass
        dx, dy, dz = x - cx, y - cy, z - cz
        radius = dx * dx + dy * dy + dz * dz
        numbers = (
            mass,
            cx,
            cy,
            cz,
            total(m * (3.0 * dx * dx - radius)),
            total(m * (3.0 * dy * dy - radius)),
            total(m * (3.0 * dz * dz - radius)),
            total(3.0 * m * dx * dy),
            total(3.0 * m * dx * dz),
            total(3.0 * m * dy * dz),
        )
        row = jnp.zeros((1, LANES), jnp.float32)
        for place, number in enumerate(numbers):
            row = jnp.where(lane == place, number, row)
        rows.append(row)
    return rows


def far_part(target, moment):
    number = [moment[:, k : k + 1] for k in range(10)]
    mass, cx, cy, cz, qxx, qyy, qzz, qxy, qxz, qyz = number
    rx, ry, rz = target[0] - cx, target[1] - cy, target[2] - cz
    square = rx * rx + ry * ry + rz * rz + softening
    inv = lax.rsqrt(square)
    inv_two = inv * inv
    inv_three = inv_two * inv
    inv_five = inv_three * inv_two
    quad_x = qxx * rx + qxy * ry + qxz * rz
    quad_y = qxy * rx + qyy * ry + qyz * rz
    quad_z = qxz * rx + qyz * ry + qzz * rz
    inner = rx * quad_x + ry * quad_y + rz * quad_z
    radial = 2.5 * inner * inv_two * inv_five - mass * inv_three
    total = lambda v: jnp.sum(v, axis=0, keepdims=True)
    return (
        total(radial * rx - quad_x * inv_five),
        total(radial * ry - quad_y * inv_five),
        total(radial * rz - quad_z * inv_five),
    )


def kernel(
    n_sec,
    n_grp,
    pos_hbm,
    vel_hbm,
    mass_hbm,
    near_hbm,
    count_hbm,
    far_hbm,
    half_out,
    vel_out,
    direct_out,
    far_out,
    pos_ref,
    vel_ref,
    mass_ref,
    near_ref,
    count_ref,
    far_ref,
    load_sem,
    ghosts,
    gathered,
    times,
    send_sem,
    recv_sem,
    moment_send,
    moment_recv,
):
    n_dev = n_sec * n_grp
    local_blocks = near_ref.shape[0]
    slots = near_ref.shape[1]
    particles = pos_ref.shape[1]
    block_size = particles // local_blocks
    group_blocks = n_sec * local_blocks
    all_blocks = n_dev * local_blocks
    sec = lax.axis_index("sec")
    grp = lax.axis_index("grp")
    me = sec * n_grp + grp

    loads = [
        pltpu.make_async_copy(source, target, load_sem.at[k])
        for k, (source, target) in enumerate(
            (
                (pos_hbm, pos_ref),
                (vel_hbm, vel_ref),
                (mass_hbm, mass_ref),
                (near_hbm, near_ref),
                (count_hbm, count_ref),
                (far_hbm, far_ref),
            )
        )
    ]
    for load in loads:
        load.start()
    barrier = pltpu.get_barrier_semaphore()

    def greet(r, carry):
        other = lax.rem(me + r, n_dev)
        pl.semaphore_signal(
            barrier,
            inc=1,
            device_id={"sec": other // n_grp, "grp": lax.rem(other, n_grp)},
            device_id_type=MESH,
        )
        return carry

    lax.fori_loop(1, n_dev, greet, 0)
    for load in loads:
        load.wait()

    number = lax.broadcasted_iota(jnp.int32, (group_blocks, slots), 0)
    slot = lax.broadcasted_iota(jnp.int32, (group_blocks, slots), 1)
    for b in range(local_blocks):
        used = jnp.where(
            (near_ref[b : b + 1, :] == number) & (slot < count_ref[b]), 1.0, 0.0
        )
        times[b] = jnp.broadcast_to(
            jnp.sum(used, axis=1, keepdims=True), (group_blocks, LANES)
        )
    entries = far_ref.shape[1]
    block_number = lax.broadcasted_iota(jnp.int32, (all_blocks, entries), 0)
    chosen = [
        jnp.where(far_ref[b : b + 1, :] == block_number, 1.0, 0.0)
        for b in range(local_blocks)
    ]

    current = pos_ref[...]
    speed = vel_ref[...]
    tiles = particles // LANES
    tiles_of_block = block_size // LANES
    for step in range(2):
        half = current + 0.5 * timestep * speed
        ghosts[step, sec, 0:3, :] = half
        ghosts[step, sec, 3:4, :] = mass_ref[...]
        if step == 0:
            pl.semaphore_wait(barrier, n_dev - 1)

        def send_particles(r, carry):
            other = lax.rem(sec + r, n_sec)
            pltpu.make_async_remote_copy(
                src_ref=ghosts.at[step, sec],
                dst_ref=ghosts.at[step, sec],
                send_sem=send_sem.at[step, other],
                recv_sem=recv_sem.at[step, sec],
                device_id={"sec": other, "grp": grp},
                device_id_type=MESH,
            ).start()
            return carry

        lax.fori_loop(1, n_sec, send_particles, 0)

        blocks = []
        for b in range(local_blocks):
            cut = slice(b * block_size, (b + 1) * block_size)
            blocks.append(
                (half[0:1, cut], half[1:2, cut], half[2:3, cut], mass_ref[0:1, cut])
            )
        for b, row in enumerate(own_moments(blocks)):
            gathered[step, me * local_blocks + b] = row

        def send_moments(r, carry):
            other = lax.rem(me + r, n_dev)
            mine = gathered.at[step, pl.ds(me * local_blocks, local_blocks)]
            pltpu.make_async_remote_copy(
                src_ref=mine,
                dst_ref=mine,
                send_sem=moment_send.at[step],
                recv_sem=moment_recv.at[step],
                device_id={"sec": other // n_grp, "grp": lax.rem(other, n_grp)},
                device_id_type=MESH,
            ).start()
            return carry

        lax.fori_loop(1, n_dev, send_moments, 0)

        def add_device(r, totals):
            other = peer(sec, r, n_sec)

            @pl.when(r > 0)
            def _():
                pltpu.make_async_copy(
                    ghosts.at[step, other], ghosts.at[step, other], recv_sem.at[step, other]
                ).wait()

            totals = [list(t) for t in totals]
            for tile in range(tiles):
                rows = ghosts[step, other, :, tile * LANES : (tile + 1) * LANES]
                columns = jnp.transpose(rows)
                place = tile // tiles_of_block
                weights = [
                    times[b, pl.ds(other * local_blocks + place, 1), :]
                    for b in range(local_blocks)
                ]
                for part in range(LANES // ROWS):
                    cut = slice(part * ROWS, (part + 1) * ROWS)
                    sx, sy, sz, sm = (
                        jnp.broadcast_to(columns[cut, c : c + 1], (ROWS, LANES)) for c in range(4)
                    )
                    scaled = [sm * w for w in weights]
                    for t in range(tiles):
                        lanes = slice(t * LANES, (t + 1) * LANES)
                        dx = sx - half[0:1, lanes]
                        dy = sy - half[1:2, lanes]
                        dz = sz - half[2:3, lanes]
                        inv = lax.rsqrt(dx * dx + dy * dy + (dz * dz + softening))
                        weight = scaled[t // tiles_of_block] * inv * (inv * inv)
                        totals[t][0] = totals[t][0] + weight * dx
                        totals[t][1] = totals[t][1] + weight * dy
                        totals[t][2] = totals[t][2] + weight * dz
            return tuple(tuple(t) for t in totals)

        zero = jnp.zeros((ROWS, LANES), jnp.float32)
        totals = lax.fori_loop(0, n_sec, add_device, tuple((zero,) * 3 for _ in range(tiles)))
        direct = jnp.concatenate(
            [
                jnp.concatenate(
                    [jnp.sum(totals[t][c], axis=0, keepdims=True) for t in range(tiles)], axis=1
                )
                for c in range(3)
            ],
            axis=0,
        )

        others = gathered.at[step, pl.ds(0, (n_dev - 1) * local_blocks)]
        pltpu.make_async_copy(others, others, moment_recv.at[step]).wait()
        table = gathered[step].reshape(all_blocks, LANES)
        far = []
        for b in range(local_blocks):
            moment = lax.dot_general(
                chosen[b],
                table,
                (((0,), (0,)), ((), ())),
                precision=lax.Precision.HIGHEST,
                preferred_element_type=jnp.float32,
            )
            cut = slice(b * block_size, (b + 1) * block_size)
            far.append(
                jnp.concatenate(
                    far_part((half[0:1, cut], half[1:2, cut], half[2:3, cut]), moment), axis=0
                )
            )
        far = jnp.concatenate(far, axis=1)
        if step == 0:
            speed = speed + timestep * (direct + far)
            current = half + 0.5 * timestep * speed
            vel_out[...] = speed
        else:
            half_out[...] = half
            direct_out[...] = direct
            far_out[...] = far

    for step in range(2):

        def sent(r, carry):
            other = lax.rem(sec + r, n_sec)
            pltpu.make_async_copy(
                ghosts.at[step, sec], ghosts.at[step, sec], send_sem.at[step, other]
            ).wait()
            return carry

        lax.fori_loop(1, n_sec, sent, 0)
        others = gathered.at[step, pl.ds(0, (n_dev - 1) * local_blocks)]
        pltpu.make_async_copy(others, others, moment_send.at[step]).wait()


def on_device(n_sec, n_grp, positions, velocities, masses, near_list, near_count, far_list):
    particles = positions.shape[1]
    local_blocks = near_list.shape[0]
    vmem = pl.BlockSpec(memory_space=pltpu.VMEM)
    half, speed, direct, far = pl.pallas_call(
        functools.partial(kernel, n_sec, n_grp),
        out_shape=[jax.ShapeDtypeStruct(positions.shape, jnp.float32)] * 4,
        in_specs=[pl.BlockSpec(memory_space=pltpu.HBM)] * 6,
        out_specs=[vmem] * 4,
        scratch_shapes=[
            pltpu.VMEM(positions.shape, jnp.float32),
            pltpu.VMEM(velocities.shape, jnp.float32),
            pltpu.VMEM((1, particles), jnp.float32),
            pltpu.VMEM(near_list.shape, jnp.int32),
            pltpu.SMEM(near_count.shape, jnp.int32),
            pltpu.VMEM(far_list.shape, jnp.int32),
            pltpu.SemaphoreType.DMA((6,)),
            pltpu.VMEM((2, n_sec, 4, particles), jnp.float32),
            pltpu.VMEM((2, n_sec * n_grp * local_blocks, 1, LANES), jnp.float32),
            pltpu.VMEM((local_blocks, n_sec * local_blocks, LANES), jnp.float32),
            pltpu.SemaphoreType.DMA((2, n_sec)),
            pltpu.SemaphoreType.DMA((2, n_sec)),
            pltpu.SemaphoreType.DMA((2,)),
            pltpu.SemaphoreType.DMA((2,)),
        ],
        compiler_params=pltpu.CompilerParams(
            collective_id=0, has_side_effects=True, vmem_limit_bytes=16 * 1024 * 1024
        ),
        name="leapfrog",
    )(*[pltpu.with_memory_space_constraint(v, pltpu.HBM) for v in (positions, velocities, masses[None, :], near_list, near_count, far_list)])
    accel = direct + far
    speed = speed + timestep * accel
    return half + 0.5 * timestep * speed, speed, accel


def solution(mesh):
    placed = (
        P(None, ("sec", "grp")),
        P(None, ("sec", "grp")),
        P(("sec", "grp")),
        P(("sec", "grp"), None),
        P(("sec", "grp")),
        P(("sec", "grp"), None),
    )
    return jax.shard_map(
        functools.partial(on_device, mesh.shape["sec"], mesh.shape["grp"]),
        mesh=mesh,
        in_specs=placed,
        out_specs=(P(None, ("sec", "grp")), P(None, ("sec", "grp")), P(None, ("sec", "grp"))),
        check_vma=False,
    )
```

```python
import functools

import jax
import jax.numpy as jnp
from jax import lax
from jax.experimental import pallas as pl
from jax.experimental.pallas import tpu as pltpu
from jax.sharding import PartitionSpec as P

timestep = 0.05
softening = 0.25
LANES = 128
ROWS = 8
PLACES = 16
UNROLL = 64
TARGET_ORDER = (0, 1, 2, 0, 1, 0, 2, 1)
SOURCE_ORDER = (0, 0, 0, 1, 1, 2, 1, 2)


def by_distance(n):
    return sorted(range(n), key=lambda b: min(b, n - b))

MESH = pl.DeviceIdType.MESH


def peer(sec, r, n_sec):
    if n_sec % 2:
        return lax.rem(sec + r, n_sec)
    pair = lax.rem(sec // 2 + r // 2, n_sec // 2)
    return pair * 2 + lax.rem(sec + r, 2)


def each_other(n_sec, n_grp, sec, grp, act):
    if n_sec * n_grp > UNROLL:

        def one(r, carry):
            other = lax.rem(sec * n_grp + grp + r, n_sec * n_grp)
            act(other // n_grp, lax.rem(other, n_grp))
            return carry

        lax.fori_loop(1, n_sec * n_grp, one, 0)
        return
    secs = [sec] + [lax.rem(sec + a, n_sec) for a in range(1, n_sec)]
    grps = [grp] + [lax.rem(grp + b, n_grp) for b in range(1, n_grp)]
    for b in by_distance(n_grp):
        for a in range(n_sec):
            if a or b:
                act(secs[a], grps[b])


def own_moments(blocks):
    width = LANES // len(blocks)
    lane = lax.broadcasted_iota(jnp.int32, (1, LANES), 1)
    place, inside = lane % PLACES, lane % width
    row = jnp.zeros((1, LANES), jnp.float32)
    middles = []
    for b, (x, y, z, m) in enumerate(blocks):
        total = lambda v: jnp.sum(v, axis=1, keepdims=True)
        mass = total(m)
        cx, cy, cz = total(m * x) / mass, total(m * y) / mass, total(m * z) / mass
        middles.append((cx, cy, cz))
        dx, dy, dz = x - cx, y - cy, z - cz
        radius = dx * dx + dy * dy + dz * dz
        numbers = (
            mass,
            cx,
            cy,
            cz,
            total(m * (3.0 * dx * dx - radius)),
            total(m * (3.0 * dy * dy - radius)),
            total(m * (3.0 * dz * dz - radius)),
            total(3.0 * m * dx * dy),
            total(3.0 * m * dx * dz),
            total(3.0 * m * dy * dz),
        )
        own = jnp.zeros((1, LANES), jnp.float32)
        for k, number in enumerate(numbers):
            own = jnp.where(place == k, number, own)
        row = jnp.where(lane // width == b, own, row)
    high = row.astype(jnp.bfloat16).astype(jnp.float32)
    rest = row - high
    middle = rest.astype(jnp.bfloat16).astype(jnp.float32)
    low = (rest - middle).astype(jnp.bfloat16).astype(jnp.float32)
    row = jnp.where(inside < PLACES, high, jnp.where(inside < 2 * PLACES, middle, low))
    return row, [sum(c) / len(blocks) for c in zip(*middles)]


def three_parts(v):
    high = v.astype(jnp.bfloat16).astype(jnp.float32)
    rest = v - high
    middle = rest.astype(jnp.bfloat16).astype(jnp.float32)
    return high, middle, rest - middle


def paired(parts, order):
    return jnp.concatenate([parts[k] for k in order], axis=0).astype(jnp.bfloat16)


def far_part(target, moment):
    number = [moment[:, k : k + 1] for k in range(10)]
    mass, cx, cy, cz, qxx, qyy, qzz, qxy, qxz, qyz = number
    rx, ry, rz = target[0] - cx, target[1] - cy, target[2] - cz
    square = rx * rx + ry * ry + rz * rz + softening
    inv = lax.rsqrt(square)
    inv_two = inv * inv
    inv_three = inv_two * inv
    inv_five = inv_three * inv_two
    quad_x = qxx * rx + qxy * ry + qxz * rz
    quad_y = qxy * rx + qyy * ry + qyz * rz
    quad_z = qxz * rx + qyz * ry + qzz * rz
    inner = rx * quad_x + ry * quad_y + rz * quad_z
    radial = 2.5 * inner * inv_two * inv_five - mass * inv_three
    total = lambda v: jnp.sum(v, axis=0, keepdims=True)
    return (
        total(radial * rx - quad_x * inv_five),
        total(radial * ry - quad_y * inv_five),
        total(radial * rz - quad_z * inv_five),
    )


def kernel(
    n_sec,
    n_grp,
    pos_hbm,
    vel_hbm,
    mass_hbm,
    near_hbm,
    count_hbm,
    far_hbm,
    half_out,
    vel_out,
    direct_out,
    far_out,
    pos_ref,
    vel_ref,
    mass_ref,
    near_ref,
    count_ref,
    far_ref,
    load_sem,
    ghosts,
    gathered,
    times,
    chosen,
    send_sem,
    recv_sem,
    moment_send,
    moment_recv,
):
    n_dev = n_sec * n_grp
    local_blocks = near_ref.shape[0]
    slots = near_ref.shape[1]
    particles = pos_ref.shape[1]
    block_size = particles // local_blocks
    group_blocks = n_sec * local_blocks
    sec = lax.axis_index("sec")
    grp = lax.axis_index("grp")
    me = sec * n_grp + grp

    loads = [
        pltpu.make_async_copy(source, target, load_sem.at[k])
        for k, (source, target) in enumerate(
            (
                (pos_hbm, pos_ref),
                (vel_hbm, vel_ref),
                (mass_hbm, mass_ref),
                (near_hbm, near_ref),
                (count_hbm, count_ref),
                (far_hbm, far_ref),
            )
        )
    ]
    for load in loads:
        load.start()
    barrier = pltpu.get_barrier_semaphore()

    def greet(to_sec, to_grp):
        pl.semaphore_signal(
            barrier, inc=1, device_id={"sec": to_sec, "grp": to_grp}, device_id_type=MESH
        )

    each_other(n_sec, n_grp, sec, grp, greet)
    for load in loads:
        load.wait()

    number = lax.broadcasted_iota(jnp.int32, (group_blocks, slots), 0)
    slot = lax.broadcasted_iota(jnp.int32, (group_blocks, slots), 1)
    for b in range(local_blocks):
        used = jnp.where(
            (near_ref[b : b + 1, :] == number) & (slot < count_ref[b]), 1.0, 0.0
        )
        times[b] = jnp.broadcast_to(
            jnp.sum(used, axis=1, keepdims=True), (group_blocks, LANES)
        )
    entries = far_ref.shape[1]
    for b in range(local_blocks):
        picked = far_ref[b : b + 1, :]
        for half_of in range(local_blocks):
            number = lax.broadcasted_iota(jnp.int32, (n_dev, entries), 0) * local_blocks + half_of
            chosen[b * entries : (b + 1) * entries, half_of * n_dev : (half_of + 1) * n_dev] = (
                jnp.transpose(jnp.where(picked == number, 1.0, 0.0))
            )

    current = pos_ref[...]
    speed = vel_ref[...]
    tiles = particles // LANES
    tiles_of_block = block_size // LANES
    for step in range(2):
        half = current + 0.5 * timestep * speed
        ghosts[step, sec, 0:3, :] = half
        ghosts[step, sec, 3:4, :] = mass_ref[...]

        blocks = []
        for b in range(local_blocks):
            cut = slice(b * block_size, (b + 1) * block_size)
            blocks.append(
                (half[0:1, cut], half[1:2, cut], half[2:3, cut], mass_ref[0:1, cut])
            )
        gathered[step, me], origin = own_moments(blocks)
        if step == 0:
            pl.semaphore_wait(barrier, n_dev - 1)
        mine = gathered.at[step, me]

        def send_moments(to_sec, to_grp):
            pltpu.make_async_remote_copy(
                src_ref=mine,
                dst_ref=mine,
                send_sem=moment_send.at[step],
                recv_sem=moment_recv.at[step],
                device_id={"sec": to_sec, "grp": to_grp},
                device_id_type=MESH,
            ).start()

        each_other(n_sec, n_grp, sec, grp, send_moments)

        for r in range(1, n_sec):
            other = lax.rem(sec + r, n_sec)
            pltpu.make_async_remote_copy(
                src_ref=ghosts.at[step, sec],
                dst_ref=ghosts.at[step, sec],
                send_sem=send_sem.at[step, other],
                recv_sem=recv_sem.at[step, sec],
                device_id={"sec": other, "grp": grp},
                device_id_type=MESH,
            ).start()

        line = lax.broadcasted_iota(jnp.int32, (ROWS, 1), 0)
        shift = jnp.where(
            line == 0, origin[0], jnp.where(line == 1, origin[1], jnp.where(line == 2, origin[2], 0.0))
        )
        near = [half[c : c + 1, :] - origin[c] for c in range(3)]
        reach = near[0] * near[0] + near[1] * near[1] + near[2] * near[2]
        one = jnp.ones_like(reach)
        target_side = paired(
            three_parts(
                jnp.concatenate(
                    [-2.0 * near[0], -2.0 * near[1], -2.0 * near[2], one, reach]
                    + [jnp.zeros_like(reach)] * 3,
                    axis=0,
                )
            ),
            TARGET_ORDER,
        )

        def add_device(r, totals):
            other = peer(sec, r, n_sec)

            @pl.when(r > 0)
            def _():
                pltpu.make_async_copy(
                    ghosts.at[step, other], ghosts.at[step, other], recv_sem.at[step, other]
                ).wait()

            totals = [list(t) for t in totals]
            for tile in range(tiles):
                rows = ghosts[step, other, :, tile * LANES : (tile + 1) * LANES]
                rows = jnp.concatenate([rows, jnp.zeros_like(rows)], axis=0) - shift
                moved = jnp.where(line < 3, rows, 0.0)
                reach = jnp.sum(moved * moved, axis=0, keepdims=True) + softening
                source_side = three_parts(
                    jnp.where(line == 3, reach, jnp.where(line == 4, 1.0, moved))
                )
                square = lax.dot_general(
                    paired(source_side, SOURCE_ORDER),
                    target_side,
                    (((0,), (0,)), ((), ())),
                    preferred_element_type=jnp.float32,
                )
                columns = jnp.transpose(rows)
                place = tile // tiles_of_block
                weights = [
                    times[b, pl.ds(other * local_blocks + place, 1), :]
                    for b in range(local_blocks)
                ]
                for part in range(LANES // ROWS):
                    cut = slice(part * ROWS, (part + 1) * ROWS)
                    sx, sy, sz, sm = (
                        jnp.broadcast_to(columns[cut, c : c + 1], (ROWS, LANES)) for c in range(4)
                    )
                    scaled = [sm * w for w in weights]
                    for t in range(tiles):
                        inv = lax.rsqrt(square[cut, t * LANES : (t + 1) * LANES])
                        weight = scaled[t // tiles_of_block] * inv * (inv * inv)
                        totals[t][0] = totals[t][0] + weight * sx
                        totals[t][1] = totals[t][1] + weight * sy
                        totals[t][2] = totals[t][2] + weight * sz
                        totals[t][3] = totals[t][3] + weight
            return tuple(tuple(t) for t in totals)

        zero = jnp.zeros((ROWS, LANES), jnp.float32)
        totals = lax.fori_loop(0, n_sec, add_device, tuple((zero,) * 4 for _ in range(tiles)))
        summed = [
            jnp.concatenate(
                [jnp.sum(totals[t][c], axis=0, keepdims=True) for t in range(tiles)], axis=1
            )
            for c in range(4)
        ]
        direct = jnp.concatenate([summed[c] - near[c] * summed[3] for c in range(3)], axis=0)

        others = gathered.at[step, pl.ds(0, n_dev - 1)]
        pltpu.make_async_copy(others, others, moment_recv.at[step]).wait()
        table = gathered[step].reshape(n_dev, LANES)
        width = LANES // local_blocks
        table = jnp.concatenate(
            [pltpu.roll(table, LANES - b * width, 1) if b else table for b in range(local_blocks)],
            axis=0,
        )
        parts = jnp.dot(
            chosen[...].astype(jnp.bfloat16),
            table.astype(jnp.bfloat16),
            preferred_element_type=jnp.float32,
        )
        parts = (
            parts
            + pltpu.roll(parts, LANES - PLACES, 1)
            + pltpu.roll(parts, LANES - 2 * PLACES, 1)
        )
        far = []
        for b in range(local_blocks):
            moment = parts[b * entries : (b + 1) * entries]
            cut = slice(b * block_size, (b + 1) * block_size)
            far.append(
                jnp.concatenate(
                    far_part((half[0:1, cut], half[1:2, cut], half[2:3, cut]), moment), axis=0
                )
            )
        far = jnp.concatenate(far, axis=1)
        if step == 0:
            speed = speed + timestep * (direct + far)
            current = half + 0.5 * timestep * speed
            vel_out[...] = speed
        else:
            half_out[...] = half
            direct_out[...] = direct
            far_out[...] = far

    for step in range(2):

        def sent(r, carry):
            other = lax.rem(sec + r, n_sec)
            pltpu.make_async_copy(
                ghosts.at[step, sec], ghosts.at[step, sec], send_sem.at[step, other]
            ).wait()
            return carry

        lax.fori_loop(1, n_sec, sent, 0)
        others = gathered.at[step, pl.ds(0, n_dev - 1)]
        pltpu.make_async_copy(others, others, moment_send.at[step]).wait()


def on_device(n_sec, n_grp, positions, velocities, masses, near_list, near_count, far_list):
    particles = positions.shape[1]
    local_blocks = near_list.shape[0]
    vmem = pl.BlockSpec(memory_space=pltpu.VMEM)
    half, speed, direct, far = pl.pallas_call(
        functools.partial(kernel, n_sec, n_grp),
        out_shape=[jax.ShapeDtypeStruct(positions.shape, jnp.float32)] * 4,
        in_specs=[pl.BlockSpec(memory_space=pltpu.HBM)] * 6,
        out_specs=[vmem] * 4,
        scratch_shapes=[
            pltpu.VMEM(positions.shape, jnp.float32),
            pltpu.VMEM(velocities.shape, jnp.float32),
            pltpu.VMEM((1, particles), jnp.float32),
            pltpu.VMEM(near_list.shape, jnp.int32),
            pltpu.SMEM(near_count.shape, jnp.int32),
            pltpu.VMEM(far_list.shape, jnp.int32),
            pltpu.SemaphoreType.DMA((6,)),
            pltpu.VMEM((2, n_sec, 4, particles), jnp.float32),
            pltpu.VMEM((2, n_sec * n_grp, 1, LANES), jnp.float32),
            pltpu.VMEM((local_blocks, n_sec * local_blocks, LANES), jnp.float32),
            pltpu.VMEM(
                (local_blocks * far_list.shape[1], n_sec * n_grp * local_blocks), jnp.float32
            ),
            pltpu.SemaphoreType.DMA((2, n_sec)),
            pltpu.SemaphoreType.DMA((2, n_sec)),
            pltpu.SemaphoreType.DMA((2,)),
            pltpu.SemaphoreType.DMA((2,)),
        ],
        compiler_params=pltpu.CompilerParams(
            collective_id=0, has_side_effects=True, vmem_limit_bytes=16 * 1024 * 1024
        ),
        name="leapfrog",
    )(*[pltpu.with_memory_space_constraint(v, pltpu.HBM) for v in (positions, velocities, masses[None, :], near_list, near_count, far_list)])
    accel = direct + far
    speed = speed + timestep * accel
    return half + 0.5 * timestep * speed, speed, accel


def solution(mesh):
    placed = (
        P(None, ("sec", "grp")),
        P(None, ("sec", "grp")),
        P(("sec", "grp")),
        P(("sec", "grp"), None),
        P(("sec", "grp")),
        P(("sec", "grp"), None),
    )
    return jax.shard_map(
        functools.partial(on_device, mesh.shape["sec"], mesh.shape["grp"]),
        mesh=mesh,
        in_specs=placed,
        out_specs=(P(None, ("sec", "grp")), P(None, ("sec", "grp")), P(None, ("sec", "grp"))),
        check_vma=False,
    )
```

```python
import functools

import jax
import jax.numpy as jnp
from jax import lax
from jax.experimental import pallas as pl
from jax.experimental.pallas import tpu as pltpu
from jax.sharding import PartitionSpec as P

timestep = 0.05
softening = 0.25
LANES = 128
ROWS = 8
NUMBERS = 10
PLACES = 16
UNROLL = 64
TARGET_ORDER = (0, 1, 2, 0, 1, 0, 2, 1)
SOURCE_ORDER = (0, 0, 0, 1, 1, 2, 1, 2)


def by_distance(n):
    return sorted(range(n), key=lambda b: min(b, n - b) if b else 1.5)

MESH = pl.DeviceIdType.MESH


def peer(sec, r, n_sec):
    if n_sec % 2:
        return lax.rem(sec + r, n_sec)
    pair = lax.rem(sec // 2 + r // 2, n_sec // 2)
    return pair * 2 + lax.rem(sec + r, 2)


def each_other(n_sec, n_grp, sec, grp, act):
    if n_sec * n_grp > UNROLL:

        def one(r, carry):
            other = lax.rem(sec * n_grp + grp + r, n_sec * n_grp)
            act(other // n_grp, lax.rem(other, n_grp))
            return carry

        lax.fori_loop(1, n_sec * n_grp, one, 0)
        return
    secs = [sec] + [lax.rem(sec + a, n_sec) for a in range(1, n_sec)]
    grps = [grp] + [lax.rem(grp + b, n_grp) for b in range(1, n_grp)]
    for b in by_distance(n_grp):
        for a in range(n_sec):
            if a or b:
                act(secs[a], grps[b])


def own_moments(blocks, about):
    width = LANES // len(blocks)
    lane = lax.broadcasted_iota(jnp.int32, (1, LANES), 1)
    place, inside = lane % PLACES, lane % width
    row = jnp.zeros((1, LANES), jnp.float32)
    middles = []
    for b, (x, y, z, m) in enumerate(blocks):
        total = lambda v: jnp.sum(v, axis=1, keepdims=True)
        mass = total(m)
        if about is None:
            px, py, pz = total(m * x) / mass, total(m * y) / mass, total(m * z) / mass
        else:
            px, py, pz = about[b]
        dx, dy, dz = x - px, y - py, z - pz
        mx, my, mz = m * dx, m * dy, m * dz
        sx, sy, sz = total(mx), total(my), total(mz)
        xx, yy, zz = total(mx * dx), total(my * dy), total(mz * dz)
        xy, xz, yz = total(mx * dy), total(mx * dz), total(my * dz)
        ox, oy, oz = sx / mass, sy / mass, sz / mass
        xx, yy, zz = xx - sx * ox, yy - sy * oy, zz - sz * oz
        xy, xz, yz = xy - sx * oy, xz - sx * oz, yz - sy * oz
        middles.append((px + ox, py + oy, pz + oz))
        numbers = (
            mass,
            *middles[-1],
            2.0 * xx - yy - zz,
            2.0 * yy - xx - zz,
            2.0 * zz - xx - yy,
            3.0 * xy,
            3.0 * xz,
            3.0 * yz,
        )
        own = jnp.zeros((1, LANES), jnp.float32)
        for k, number in enumerate(numbers):
            own = jnp.where(place == k, number, own)
        row = jnp.where(lane // width == b, own, row)
    high = row.astype(jnp.bfloat16).astype(jnp.float32)
    rest = row - high
    middle = rest.astype(jnp.bfloat16).astype(jnp.float32)
    low = (rest - middle).astype(jnp.bfloat16).astype(jnp.float32)
    row = jnp.where(inside < PLACES, high, jnp.where(inside < 2 * PLACES, middle, low))
    return row, middles


def three_parts(v):
    high = v.astype(jnp.bfloat16).astype(jnp.float32)
    rest = v - high
    middle = rest.astype(jnp.bfloat16).astype(jnp.float32)
    return high, middle, rest - middle


def paired(parts, order):
    return jnp.concatenate([parts[k] for k in order], axis=0).astype(jnp.bfloat16)


def far_part(target, moment):
    mass, cx, cy, cz, qxx, qyy, qzz, qxy, qxz, qyz = moment
    rx, ry, rz = target[0] - cx, target[1] - cy, target[2] - cz
    square = rx * rx + ry * ry + rz * rz + softening
    inv = lax.rsqrt(square)
    inv_two = inv * inv
    inv_five = inv_two * inv_two * inv
    quad_x = qxx * rx + qxy * ry + qxz * rz
    quad_y = qxy * rx + qyy * ry + qyz * rz
    quad_z = qxz * rx + qyz * ry + qzz * rz
    inner = rx * quad_x + ry * quad_y + rz * quad_z
    radial = 2.5 * inner * inv_two - mass * square
    total = lambda v: jnp.sum(v, axis=0, keepdims=True)
    return (
        total((radial * rx - quad_x) * inv_five),
        total((radial * ry - quad_y) * inv_five),
        total((radial * rz - quad_z) * inv_five),
    )


def kernel(
    n_sec,
    n_grp,
    pos_hbm,
    vel_hbm,
    mass_hbm,
    near_hbm,
    count_hbm,
    far_hbm,
    half_out,
    vel_out,
    direct_out,
    far_out,
    pos_ref,
    vel_ref,
    mass_ref,
    near_ref,
    count_ref,
    far_ref,
    load_sem,
    ghosts,
    gathered,
    times,
    chosen,
    spread,
    target_side,
    send_sem,
    recv_sem,
    moment_send,
    moment_recv,
):
    n_dev = n_sec * n_grp
    local_blocks = near_ref.shape[0]
    slots = near_ref.shape[1]
    particles = pos_ref.shape[1]
    block_size = particles // local_blocks
    group_blocks = n_sec * local_blocks
    sec = lax.axis_index("sec")
    grp = lax.axis_index("grp")
    me = sec * n_grp + grp

    loads = [
        pltpu.make_async_copy(source, target, load_sem.at[k])
        for k, (source, target) in enumerate(
            (
                (pos_hbm, pos_ref),
                (vel_hbm, vel_ref),
                (mass_hbm, mass_ref),
                (near_hbm, near_ref),
                (count_hbm, count_ref),
                (far_hbm, far_ref),
            )
        )
    ]
    for load in loads:
        load.start()
    barrier = pltpu.get_barrier_semaphore()

    def greet(to_sec, to_grp):
        pl.semaphore_signal(
            barrier, inc=1, device_id={"sec": to_sec, "grp": to_grp}, device_id_type=MESH
        )

    each_other(n_sec, n_grp, sec, grp, greet)
    for load in loads:
        load.wait()

    number = lax.broadcasted_iota(jnp.int32, (group_blocks, slots), 0)
    slot = lax.broadcasted_iota(jnp.int32, (group_blocks, slots), 1)
    for b in range(local_blocks):
        used = jnp.where(
            (near_ref[b : b + 1, :] == number) & (slot < count_ref[b]), 1.0, 0.0
        )
        times[b] = jnp.broadcast_to(
            jnp.sum(used, axis=1, keepdims=True), (group_blocks, LANES)
        )
    entries = far_ref.shape[1]
    for b in range(local_blocks):
        picked = far_ref[b : b + 1, :]
        for half_of in range(local_blocks):
            number = lax.broadcasted_iota(jnp.int32, (n_dev, entries), 0) * local_blocks + half_of
            chosen[b * entries : (b + 1) * entries, half_of * n_dev : (half_of + 1) * n_dev] = (
                jnp.transpose(jnp.where(picked == number, 1.0, 0.0))
            )

    middles = None
    current = pos_ref[...]
    speed = vel_ref[...]
    source_lane = lax.broadcasted_iota(jnp.int32, (LANES, LANES), 0)
    for k in range(NUMBERS):
        spread[:, k * LANES : (k + 1) * LANES] = jnp.where(
            (source_lane % PLACES == k) & (source_lane < 3 * PLACES), 1.0, 0.0
        ).astype(jnp.bfloat16)
    tiles = particles // LANES
    tiles_of_block = block_size // LANES
    for step in range(2):
        half = current + 0.5 * timestep * speed
        ghosts[step, sec, 0:3, :] = half
        ghosts[step, sec, 3:4, :] = mass_ref[...]

        blocks = []
        for b in range(local_blocks):
            cut = slice(b * block_size, (b + 1) * block_size)
            blocks.append(
                (half[0:1, cut], half[1:2, cut], half[2:3, cut], mass_ref[0:1, cut])
            )
        gathered[step, me], middles = own_moments(blocks, middles)
        origin = [sum(c) / local_blocks for c in zip(*middles)]
        if step == 0:
            pl.semaphore_wait(barrier, n_dev - 1)
        mine = gathered.at[step, me]

        def send_moments(to_sec, to_grp):
            pltpu.make_async_remote_copy(
                src_ref=mine,
                dst_ref=mine,
                send_sem=moment_send.at[step],
                recv_sem=moment_recv.at[step],
                device_id={"sec": to_sec, "grp": to_grp},
                device_id_type=MESH,
            ).start()

        each_other(n_sec, n_grp, sec, grp, send_moments)

        for r in range(1, n_sec):
            other = lax.rem(sec + r, n_sec)
            pltpu.make_async_remote_copy(
                src_ref=ghosts.at[step, sec],
                dst_ref=ghosts.at[step, sec],
                send_sem=send_sem.at[step, other],
                recv_sem=recv_sem.at[step, sec],
                device_id={"sec": other, "grp": grp},
                device_id_type=MESH,
            ).start()

        line = lax.broadcasted_iota(jnp.int32, (ROWS, 1), 0)
        shift = jnp.where(
            line == 0, origin[0], jnp.where(line == 1, origin[1], jnp.where(line == 2, origin[2], 0.0))
        )

        @pl.when(sec >= 0)
        def _():
            near = [half[c : c + 1, :] - origin[c] for c in range(3)]
            reach = near[0] * near[0] + near[1] * near[1] + near[2] * near[2]
            target_side[...] = paired(
                three_parts(
                    jnp.concatenate(
                        [-2.0 * near[0], -2.0 * near[1], -2.0 * near[2], jnp.ones_like(reach), reach]
                        + [jnp.zeros_like(reach)] * 3,
                        axis=0,
                    )
                ),
                TARGET_ORDER,
            )

        def add_device(r, totals):
            other = peer(sec, r, n_sec)

            @pl.when(r > 0)
            def _():
                pltpu.make_async_copy(
                    ghosts.at[step, other], ghosts.at[step, other], recv_sem.at[step, other]
                ).wait()

            totals = [list(t) for t in totals]
            for tile in range(tiles):
                rows = ghosts[step, other, :, tile * LANES : (tile + 1) * LANES]
                rows = jnp.concatenate([rows, jnp.zeros_like(rows)], axis=0) - shift
                moved = jnp.where(line < 3, rows, 0.0)
                reach = jnp.sum(moved * moved, axis=0, keepdims=True) + softening
                source_side = three_parts(
                    jnp.where(line == 3, reach, jnp.where(line == 4, 1.0, moved))
                )
                square = lax.dot_general(
                    paired(source_side, SOURCE_ORDER),
                    target_side[...],
                    (((0,), (0,)), ((), ())),
                    preferred_element_type=jnp.float32,
                )
                columns = jnp.transpose(rows)
                place = tile // tiles_of_block
                weights = [
                    times[b, pl.ds(other * local_blocks + place, 1), :]
                    for b in range(local_blocks)
                ]
                for part in range(LANES // ROWS):
                    cut = slice(part * ROWS, (part + 1) * ROWS)
                    sx, sy, sz, sm = (
                        jnp.broadcast_to(columns[cut, c : c + 1], (ROWS, LANES)) for c in range(4)
                    )
                    scaled = [sm * w for w in weights]
                    for t in range(tiles):
                        inv = lax.rsqrt(square[cut, t * LANES : (t + 1) * LANES])
                        weight = scaled[t // tiles_of_block] * inv * (inv * inv)
                        totals[t][0] = totals[t][0] + weight * sx
                        totals[t][1] = totals[t][1] + weight * sy
                        totals[t][2] = totals[t][2] + weight * sz
                        totals[t][3] = totals[t][3] + weight
            return tuple(tuple(t) for t in totals)

        zero = jnp.zeros((ROWS, LANES), jnp.float32)
        totals = lax.fori_loop(0, n_sec, add_device, tuple((zero,) * 4 for _ in range(tiles)))
        summed = [
            jnp.concatenate(
                [jnp.sum(totals[t][c], axis=0, keepdims=True) for t in range(tiles)], axis=1
            )
            for c in range(4)
        ]
        direct = jnp.concatenate(
            [summed[c] - (half[c : c + 1, :] - origin[c]) * summed[3] for c in range(3)], axis=0
        )

        others = gathered.at[step, pl.ds(0, n_dev - 1)]
        for r in range(1, n_sec):
            pltpu.make_async_copy(
                ghosts.at[step, sec], ghosts.at[step, sec], send_sem.at[step, lax.rem(sec + r, n_sec)]
            ).wait()
        pltpu.make_async_copy(others, others, moment_send.at[step]).wait()
        pltpu.make_async_copy(others, others, moment_recv.at[step]).wait()
        table = gathered[step].reshape(n_dev, LANES)
        width = LANES // local_blocks
        table = jnp.concatenate(
            [pltpu.roll(table, LANES - b * width, 1) if b else table for b in range(local_blocks)],
            axis=0,
        )
        parts = jnp.dot(
            chosen[...].astype(jnp.bfloat16),
            table.astype(jnp.bfloat16),
            preferred_element_type=jnp.float32,
        )
        numbers = jnp.dot(
            parts.astype(jnp.bfloat16), spread[...], preferred_element_type=jnp.float32
        )
        far = []
        for b in range(local_blocks):
            moment = [
                jnp.concatenate(
                    [numbers[b * entries : (b + 1) * entries, k * LANES : (k + 1) * LANES]]
                    * tiles_of_block,
                    axis=1,
                )
                for k in range(NUMBERS)
            ]
            cut = slice(b * block_size, (b + 1) * block_size)
            far.append(
                jnp.concatenate(
                    far_part((half[0:1, cut], half[1:2, cut], half[2:3, cut]), moment), axis=0
                )
            )
        far = jnp.concatenate(far, axis=1)
        if step == 0:
            speed = speed + timestep * (direct + far)
            current = half + 0.5 * timestep * speed
            vel_out[...] = speed
        else:
            half_out[...] = half
            direct_out[...] = direct
            far_out[...] = far


def on_device(n_sec, n_grp, positions, velocities, masses, near_list, near_count, far_list):
    particles = positions.shape[1]
    local_blocks = near_list.shape[0]
    vmem = pl.BlockSpec(memory_space=pltpu.VMEM)
    half, speed, direct, far = pl.pallas_call(
        functools.partial(kernel, n_sec, n_grp),
        out_shape=[jax.ShapeDtypeStruct(positions.shape, jnp.float32)] * 4,
        in_specs=[pl.BlockSpec(memory_space=pltpu.HBM)] * 6,
        out_specs=[vmem] * 4,
        scratch_shapes=[
            pltpu.VMEM(positions.shape, jnp.float32),
            pltpu.VMEM(velocities.shape, jnp.float32),
            pltpu.VMEM((1, particles), jnp.float32),
            pltpu.VMEM(near_list.shape, jnp.int32),
            pltpu.SMEM(near_count.shape, jnp.int32),
            pltpu.VMEM(far_list.shape, jnp.int32),
            pltpu.SemaphoreType.DMA((6,)),
            pltpu.VMEM((2, n_sec, 4, particles), jnp.float32),
            pltpu.VMEM((2, n_sec * n_grp, 1, LANES), jnp.float32),
            pltpu.VMEM((local_blocks, n_sec * local_blocks, LANES), jnp.float32),
            pltpu.VMEM(
                (local_blocks * far_list.shape[1], n_sec * n_grp * local_blocks), jnp.float32
            ),
            pltpu.VMEM((LANES, NUMBERS * LANES), jnp.bfloat16),
            pltpu.VMEM((len(TARGET_ORDER) * ROWS, particles), jnp.bfloat16),
            pltpu.SemaphoreType.DMA((2, n_sec)),
            pltpu.SemaphoreType.DMA((2, n_sec)),
            pltpu.SemaphoreType.DMA((2,)),
            pltpu.SemaphoreType.DMA((2,)),
        ],
        compiler_params=pltpu.CompilerParams(
            collective_id=0, has_side_effects=True, vmem_limit_bytes=16 * 1024 * 1024
        ),
        name="leapfrog",
    )(*[pltpu.with_memory_space_constraint(v, pltpu.HBM) for v in (positions, velocities, masses[None, :], near_list, near_count, far_list)])
    accel = direct + far
    speed = speed + timestep * accel
    return half + 0.5 * timestep * speed, speed, accel


def solution(mesh):
    placed = (
        P(None, ("sec", "grp")),
        P(None, ("sec", "grp")),
        P(("sec", "grp")),
        P(("sec", "grp"), None),
        P(("sec", "grp")),
        P(("sec", "grp"), None),
    )
    return jax.shard_map(
        functools.partial(on_device, mesh.shape["sec"], mesh.shape["grp"]),
        mesh=mesh,
        in_specs=placed,
        out_specs=(P(None, ("sec", "grp")), P(None, ("sec", "grp")), P(None, ("sec", "grp"))),
        check_vma=False,
    )
```

```python
import functools

import jax
import jax.numpy as jnp
from jax import lax
from jax.experimental import pallas as pl
from jax.experimental.pallas import tpu as pltpu
from jax.sharding import PartitionSpec as P

timestep = 0.05
softening = 0.25
LANES = 128
ROWS = 8
NUMBERS = 10
PLACES = 16
UNROLL = 64
TARGET_ORDER = (0, 1, 2, 0, 1, 0, 2, 1)
SOURCE_ORDER = (0, 0, 0, 1, 1, 2, 1, 2)


def by_distance(n):
    return sorted(range(n), key=lambda b: min(b, n - b) if b else 1.5)

MESH = pl.DeviceIdType.MESH


def peer(sec, r, n_sec):
    if n_sec % 2:
        return lax.rem(sec + r, n_sec)
    pair = lax.rem(sec // 2 + r // 2, n_sec // 2)
    return pair * 2 + lax.rem(sec + r, 2)


def each_other(n_sec, n_grp, sec, grp, act):
    if n_sec * n_grp > UNROLL:

        def one(r, carry):
            other = lax.rem(sec * n_grp + grp + r, n_sec * n_grp)
            act(other // n_grp, lax.rem(other, n_grp))
            return carry

        lax.fori_loop(1, n_sec * n_grp, one, 0)
        return
    secs = [sec] + [lax.rem(sec + a, n_sec) for a in range(1, n_sec)]
    grps = [grp] + [lax.rem(grp + b, n_grp) for b in range(1, n_grp)]
    for b in by_distance(n_grp):
        for a in range(n_sec):
            if a or b:
                act(secs[a], grps[b])


def own_moments(blocks, about):
    width = LANES // len(blocks)
    lane = lax.broadcasted_iota(jnp.int32, (1, LANES), 1)
    place, inside = lane % PLACES, lane % width
    row = jnp.zeros((1, LANES), jnp.float32)
    middles = []
    for b, (x, y, z, m) in enumerate(blocks):
        total = lambda v: jnp.sum(v, axis=1, keepdims=True)
        mass = total(m)
        if about is None:
            px, py, pz = total(m * x) / mass, total(m * y) / mass, total(m * z) / mass
        else:
            px, py, pz = about[b]
        dx, dy, dz = x - px, y - py, z - pz
        mx, my, mz = m * dx, m * dy, m * dz
        sx, sy, sz = total(mx), total(my), total(mz)
        xx, yy, zz = total(mx * dx), total(my * dy), total(mz * dz)
        xy, xz, yz = total(mx * dy), total(mx * dz), total(my * dz)
        ox, oy, oz = sx / mass, sy / mass, sz / mass
        xx, yy, zz = xx - sx * ox, yy - sy * oy, zz - sz * oz
        xy, xz, yz = xy - sx * oy, xz - sx * oz, yz - sy * oz
        middles.append((px + ox, py + oy, pz + oz))
        numbers = (
            mass,
            *middles[-1],
            2.0 * xx - yy - zz,
            2.0 * yy - xx - zz,
            2.0 * zz - xx - yy,
            3.0 * xy,
            3.0 * xz,
            3.0 * yz,
        )
        own = jnp.zeros((1, LANES), jnp.float32)
        for k, number in enumerate(numbers):
            own = jnp.where(place == k, number, own)
        row = jnp.where(lane // width == b, own, row)
    high = row.astype(jnp.bfloat16).astype(jnp.float32)
    rest = row - high
    middle = rest.astype(jnp.bfloat16).astype(jnp.float32)
    low = (rest - middle).astype(jnp.bfloat16).astype(jnp.float32)
    row = jnp.where(inside < PLACES, high, jnp.where(inside < 2 * PLACES, middle, low))
    return row, middles


def three_parts(v):
    high = v.astype(jnp.bfloat16).astype(jnp.float32)
    rest = v - high
    middle = rest.astype(jnp.bfloat16).astype(jnp.float32)
    return high, middle, rest - middle


def paired(parts, order):
    return jnp.concatenate([parts[k] for k in order], axis=0).astype(jnp.bfloat16)


def far_part(target, moment):
    mass, cx, cy, cz, qxx, qyy, qzz, qxy, qxz, qyz = moment
    rx, ry, rz = target[0] - cx, target[1] - cy, target[2] - cz
    square = rx * rx + ry * ry + rz * rz + softening
    inv = lax.rsqrt(square)
    inv_two = inv * inv
    inv_five = inv_two * inv_two * inv
    quad_x = qxx * rx + qxy * ry + qxz * rz
    quad_y = qxy * rx + qyy * ry + qyz * rz
    quad_z = qxz * rx + qyz * ry + qzz * rz
    inner = rx * quad_x + ry * quad_y + rz * quad_z
    radial = 2.5 * inner * inv_two - mass * square
    total = lambda v: jnp.sum(v, axis=0, keepdims=True)
    return (
        total((radial * rx - quad_x) * inv_five),
        total((radial * ry - quad_y) * inv_five),
        total((radial * rz - quad_z) * inv_five),
    )


def kernel(
    n_sec,
    n_grp,
    pos_hbm,
    vel_hbm,
    mass_hbm,
    near_hbm,
    count_hbm,
    far_hbm,
    half_out,
    vel_out,
    direct_out,
    far_out,
    pos_ref,
    vel_ref,
    mass_ref,
    near_ref,
    count_ref,
    far_ref,
    ghosts,
    gathered,
    times,
    chosen,
    kept,
    spread,
    target_side,
    send_sem,
    recv_sem,
    moment_recv,
):
    n_dev = n_sec * n_grp
    local_blocks = near_ref.shape[0]
    slots = near_ref.shape[1]
    particles = pos_ref.shape[1]
    block_size = particles // local_blocks
    group_blocks = n_sec * local_blocks
    sec = lax.axis_index("sec")
    grp = lax.axis_index("grp")
    me = sec * n_grp + grp

    barrier = pltpu.get_barrier_semaphore()

    def take(load_sem):
        loads = [
            pltpu.make_async_copy(source, target, load_sem.at[k])
            for k, (source, target) in enumerate(
                (
                    (pos_hbm, pos_ref),
                    (vel_hbm, vel_ref),
                    (mass_hbm, mass_ref),
                    (near_hbm, near_ref),
                    (count_hbm, count_ref),
                    (far_hbm, far_ref),
                )
            )
        ]
        for load in loads:
            load.start()

        def greet(to_sec, to_grp):
            pl.semaphore_signal(
                barrier, inc=1, device_id={"sec": to_sec, "grp": to_grp}, device_id_type=MESH
            )

        each_other(n_sec, n_grp, sec, grp, greet)
        for load in loads:
            load.wait()

    pl.run_scoped(take, pltpu.SemaphoreType.DMA((6,)))

    number = lax.broadcasted_iota(jnp.int32, (group_blocks, slots), 0)
    slot = lax.broadcasted_iota(jnp.int32, (group_blocks, slots), 1)
    for b in range(local_blocks):
        used = jnp.where(
            (near_ref[b : b + 1, :] == number) & (slot < count_ref[b]), 1.0, 0.0
        )
        times[b] = jnp.broadcast_to(
            jnp.sum(used, axis=1, keepdims=True), (group_blocks, LANES)
        )
    entries = far_ref.shape[1]
    width = LANES // local_blocks
    half_of_lane = lax.broadcasted_iota(jnp.int32, (entries, LANES), 1) // width
    number = lax.broadcasted_iota(jnp.int32, (n_dev, entries), 0)
    for b in range(local_blocks):
        rows = slice(b * entries, (b + 1) * entries)
        picked = far_ref[b : b + 1, :]
        chosen[rows, :] = jnp.transpose(jnp.where(picked // local_blocks == number, 1.0, 0.0))
        place = jnp.transpose(
            jnp.broadcast_to((picked % local_blocks).astype(jnp.float32), (LANES, entries))
        )
        kept[rows, :] = jnp.where(place == half_of_lane.astype(jnp.float32), 1.0, 0.0)

    middles = None
    current = pos_ref[...]
    speed = vel_ref[...]

    source_lane = lax.broadcasted_iota(jnp.int32, (LANES, LANES), 0)
    for k in range(NUMBERS):
        spread[:, k * LANES : (k + 1) * LANES] = jnp.where(
            (source_lane % PLACES == k) & (source_lane % width < 3 * PLACES), 1.0, 0.0
        ).astype(jnp.bfloat16)
    tiles = particles // LANES
    tiles_of_block = block_size // LANES
    for step in range(2):
        half = current + 0.5 * timestep * speed
        ghosts[step, sec, 0:3, :] = half
        ghosts[step, sec, 3:4, :] = mass_ref[...]

        blocks = []
        for b in range(local_blocks):
            cut = slice(b * block_size, (b + 1) * block_size)
            blocks.append(
                (half[0:1, cut], half[1:2, cut], half[2:3, cut], mass_ref[0:1, cut])
            )
        gathered[step, me], middles = own_moments(blocks, middles)
        origin = [sum(c) / local_blocks for c in zip(*middles)]
        if step == 0:
            pl.semaphore_wait(barrier, n_dev - 1)
        mine = gathered.at[step, me]

        def send_moments(to_sec, to_grp):
            pltpu.make_async_remote_copy(
                src_ref=mine,
                dst_ref=mine,
                send_sem=send_sem.at[1],
                recv_sem=moment_recv.at[step],
                device_id={"sec": to_sec, "grp": to_grp},
                device_id_type=MESH,
            ).start()

        each_other(n_sec, n_grp, sec, grp, send_moments)

        for r in range(1, n_sec):
            other = lax.rem(sec + r, n_sec)
            pltpu.make_async_remote_copy(
                src_ref=ghosts.at[step, sec],
                dst_ref=ghosts.at[step, sec],
                send_sem=send_sem.at[0],
                recv_sem=recv_sem.at[step, r - 1],
                device_id={"sec": other, "grp": grp},
                device_id_type=MESH,
            ).start()

        line = lax.broadcasted_iota(jnp.int32, (ROWS, 1), 0)
        shift = jnp.where(
            line == 0, origin[0], jnp.where(line == 1, origin[1], jnp.where(line == 2, origin[2], 0.0))
        )

        @pl.when(sec >= 0)
        def _():
            near = [half[c : c + 1, :] - origin[c] for c in range(3)]
            reach = near[0] * near[0] + near[1] * near[1] + near[2] * near[2]
            target_side[...] = paired(
                three_parts(
                    jnp.concatenate(
                        [-2.0 * near[0], -2.0 * near[1], -2.0 * near[2], jnp.ones_like(reach), reach]
                        + [jnp.zeros_like(reach)] * 3,
                        axis=0,
                    )
                ),
                TARGET_ORDER,
            )

        def add_device(r, totals):
            other = peer(sec, r, n_sec)

            @pl.when(r > 0)
            def _():
                pltpu.make_async_copy(
                    ghosts.at[step, other],
                    ghosts.at[step, other],
                    recv_sem.at[step, lax.rem(sec - other + n_sec, n_sec) - 1],
                ).wait()

            totals = [list(t) for t in totals]
            for tile in range(tiles):
                rows = ghosts[step, other, :, tile * LANES : (tile + 1) * LANES]
                rows = jnp.concatenate([rows, jnp.zeros_like(rows)], axis=0) - shift
                moved = jnp.where(line < 3, rows, 0.0)
                reach = jnp.sum(moved * moved, axis=0, keepdims=True) + softening
                source_side = three_parts(
                    jnp.where(line == 3, reach, jnp.where(line == 4, 1.0, moved))
                )
                square = lax.dot_general(
                    paired(source_side, SOURCE_ORDER),
                    target_side[...],
                    (((0,), (0,)), ((), ())),
                    preferred_element_type=jnp.float32,
                )
                columns = jnp.transpose(rows)
                place = tile // tiles_of_block
                weights = [
                    times[b, pl.ds(other * local_blocks + place, 1), :]
                    for b in range(local_blocks)
                ]
                for part in range(LANES // ROWS):
                    cut = slice(part * ROWS, (part + 1) * ROWS)
                    sx, sy, sz, sm = (
                        jnp.broadcast_to(columns[cut, c : c + 1], (ROWS, LANES)) for c in range(4)
                    )
                    scaled = [sm * w for w in weights]
                    for t in range(tiles):
                        inv = lax.rsqrt(square[cut, t * LANES : (t + 1) * LANES])
                        weight = scaled[t // tiles_of_block] * inv * (inv * inv)
                        totals[t][0] = totals[t][0] + weight * sx
                        totals[t][1] = totals[t][1] + weight * sy
                        totals[t][2] = totals[t][2] + weight * sz
                        totals[t][3] = totals[t][3] + weight
            return tuple(tuple(t) for t in totals)

        zero = jnp.zeros((ROWS, LANES), jnp.float32)
        totals = lax.fori_loop(0, n_sec, add_device, tuple((zero,) * 4 for _ in range(tiles)))
        summed = [
            jnp.concatenate(
                [jnp.sum(totals[t][c], axis=0, keepdims=True) for t in range(tiles)], axis=1
            )
            for c in range(4)
        ]
        direct = jnp.concatenate(
            [summed[c] - (half[c : c + 1, :] - origin[c]) * summed[3] for c in range(3)], axis=0
        )

        others = gathered.at[step, pl.ds(0, n_dev - 1)]
        sent = ghosts.at[step, pl.ds(0, n_sec - 1)]
        pltpu.make_async_copy(sent, sent, send_sem.at[0]).wait()
        pltpu.make_async_copy(others, others, send_sem.at[1]).wait()
        pltpu.make_async_copy(others, others, moment_recv.at[step]).wait()
        table = gathered[step].reshape(n_dev, LANES)
        parts = jnp.dot(
            chosen[...].astype(jnp.bfloat16),
            table.astype(jnp.bfloat16),
            preferred_element_type=jnp.float32,
        )
        numbers = jnp.dot(
            (parts * kept[...]).astype(jnp.bfloat16), spread[...], preferred_element_type=jnp.float32
        )
        far = []
        for b in range(local_blocks):
            moment = [
                jnp.concatenate(
                    [numbers[b * entries : (b + 1) * entries, k * LANES : (k + 1) * LANES]]
                    * tiles_of_block,
                    axis=1,
                )
                for k in range(NUMBERS)
            ]
            cut = slice(b * block_size, (b + 1) * block_size)
            far.append(
                jnp.concatenate(
                    far_part((half[0:1, cut], half[1:2, cut], half[2:3, cut]), moment), axis=0
                )
            )
        far = jnp.concatenate(far, axis=1)
        if step == 0:
            speed = speed + timestep * (direct + far)
            current = half + 0.5 * timestep * speed
            vel_out[...] = speed
        else:
            half_out[...] = half
            direct_out[...] = direct
            far_out[...] = far


def on_device(n_sec, n_grp, positions, velocities, masses, near_list, near_count, far_list):
    particles = positions.shape[1]
    local_blocks = near_list.shape[0]
    vmem = pl.BlockSpec(memory_space=pltpu.VMEM)
    half, speed, direct, far = pl.pallas_call(
        functools.partial(kernel, n_sec, n_grp),
        out_shape=[jax.ShapeDtypeStruct(positions.shape, jnp.float32)] * 4,
        in_specs=[pl.BlockSpec(memory_space=pltpu.HBM)] * 6,
        out_specs=[vmem] * 4,
        scratch_shapes=[
            pltpu.VMEM(positions.shape, jnp.float32),
            pltpu.VMEM(velocities.shape, jnp.float32),
            pltpu.VMEM((1, particles), jnp.float32),
            pltpu.VMEM(near_list.shape, jnp.int32),
            pltpu.SMEM(near_count.shape, jnp.int32),
            pltpu.VMEM(far_list.shape, jnp.int32),
            pltpu.VMEM((2, n_sec, 4, particles), jnp.float32),
            pltpu.VMEM((2, n_sec * n_grp, 1, LANES), jnp.float32),
            pltpu.VMEM((local_blocks, n_sec * local_blocks, LANES), jnp.float32),
            pltpu.VMEM(
                (local_blocks * far_list.shape[1], n_sec * n_grp), jnp.float32
            ),
            pltpu.VMEM((local_blocks * far_list.shape[1], LANES), jnp.float32),
            pltpu.VMEM((LANES, NUMBERS * LANES), jnp.bfloat16),
            pltpu.VMEM((len(TARGET_ORDER) * ROWS, particles), jnp.bfloat16),
            pltpu.SemaphoreType.DMA((2,)),
            pltpu.SemaphoreType.DMA((2, n_sec - 1)),
            pltpu.SemaphoreType.DMA((2,)),
        ],
        compiler_params=pltpu.CompilerParams(
            collective_id=0, has_side_effects=True, vmem_limit_bytes=16 * 1024 * 1024
        ),
        name="leapfrog",
    )(*[pltpu.with_memory_space_constraint(v, pltpu.HBM) for v in (positions, velocities, masses[None, :], near_list, near_count, far_list)])
    accel = direct + far
    speed = speed + timestep * accel
    return half + 0.5 * timestep * speed, speed, accel


def solution(mesh):
    placed = (
        P(None, ("sec", "grp")),
        P(None, ("sec", "grp")),
        P(("sec", "grp")),
        P(("sec", "grp"), None),
        P(("sec", "grp")),
        P(("sec", "grp"), None),
    )
    return jax.shard_map(
        functools.partial(on_device, mesh.shape["sec"], mesh.shape["grp"]),
        mesh=mesh,
        in_specs=placed,
        out_specs=(P(None, ("sec", "grp")), P(None, ("sec", "grp")), P(None, ("sec", "grp"))),
        check_vma=False,
    )
```

```python
import functools

import jax
import jax.numpy as jnp
from jax import lax
from jax.experimental import pallas as pl
from jax.experimental.pallas import tpu as pltpu
from jax.sharding import PartitionSpec as P

timestep = 0.05
softening = 0.25
LANES = 128
ROWS = 8
NUMBERS = 10
PLACES = 16
UNROLL = 64
TARGET_ORDER = (0, 1, 2, 0, 1, 0, 2, 1)
SOURCE_ORDER = (0, 0, 0, 1, 1, 2, 1, 2)


def by_distance(n):
    return sorted(range(n), key=lambda b: min(b, n - b) if b else 2.5)

MESH = pl.DeviceIdType.MESH


def peer(sec, r, n_sec):
    if n_sec % 2:
        return lax.rem(sec + r, n_sec)
    pair = lax.rem(sec // 2 + r // 2, n_sec // 2)
    return pair * 2 + lax.rem(sec + r, 2)


def each_other(n_sec, n_grp, sec, grp, act):
    if n_sec * n_grp > UNROLL:

        def one(r, carry):
            other = lax.rem(sec * n_grp + grp + r, n_sec * n_grp)
            act(other // n_grp, lax.rem(other, n_grp))
            return carry

        lax.fori_loop(1, n_sec * n_grp, one, 0)
        return
    secs = [sec] + [lax.rem(sec + a, n_sec) for a in range(1, n_sec)]
    grps = [grp] + [lax.rem(grp + b, n_grp) for b in range(1, n_grp)]
    for b in by_distance(n_grp):
        for a in range(n_sec - 1, -1, -1):
            if a or b:
                act(secs[a], grps[b])


def own_moments(blocks, about):
    width = LANES // len(blocks)
    lane = lax.broadcasted_iota(jnp.int32, (1, LANES), 1)
    place, inside = lane % PLACES, lane % width
    row = jnp.zeros((1, LANES), jnp.float32)
    middles = []
    for b, (x, y, z, m) in enumerate(blocks):
        total = lambda v: jnp.sum(v, axis=1, keepdims=True)
        mass = total(m)
        if about is None:
            px, py, pz = total(m * x) / mass, total(m * y) / mass, total(m * z) / mass
        else:
            px, py, pz = about[b]
        dx, dy, dz = x - px, y - py, z - pz
        mx, my, mz = m * dx, m * dy, m * dz
        sx, sy, sz = total(mx), total(my), total(mz)
        xx, yy, zz = total(mx * dx), total(my * dy), total(mz * dz)
        xy, xz, yz = total(mx * dy), total(mx * dz), total(my * dz)
        ox, oy, oz = sx / mass, sy / mass, sz / mass
        xx, yy, zz = xx - sx * ox, yy - sy * oy, zz - sz * oz
        xy, xz, yz = xy - sx * oy, xz - sx * oz, yz - sy * oz
        middles.append((px + ox, py + oy, pz + oz))
        numbers = (
            mass,
            *middles[-1],
            2.0 * xx - yy - zz,
            2.0 * yy - xx - zz,
            2.0 * zz - xx - yy,
            3.0 * xy,
            3.0 * xz,
            3.0 * yz,
        )
        own = jnp.zeros((1, LANES), jnp.float32)
        for k, number in enumerate(numbers):
            own = jnp.where(place == k, number, own)
        row = jnp.where(lane // width == b, own, row)
    high = row.astype(jnp.bfloat16).astype(jnp.float32)
    rest = row - high
    middle = rest.astype(jnp.bfloat16).astype(jnp.float32)
    low = (rest - middle).astype(jnp.bfloat16).astype(jnp.float32)
    row = jnp.where(inside < PLACES, high, jnp.where(inside < 2 * PLACES, middle, low))
    return row, middles


def three_parts(v):
    high = v.astype(jnp.bfloat16).astype(jnp.float32)
    rest = v - high
    middle = rest.astype(jnp.bfloat16).astype(jnp.float32)
    return high, middle, rest - middle


def paired(parts, order):
    return jnp.concatenate([parts[k] for k in order], axis=0).astype(jnp.bfloat16)


def far_part(target, moment):
    mass, cx, cy, cz, qxx, qyy, qzz, qxy, qxz, qyz = moment
    rx, ry, rz = target[0] - cx, target[1] - cy, target[2] - cz
    square = rx * rx + ry * ry + rz * rz + softening
    inv = lax.rsqrt(square)
    inv_two = inv * inv
    inv_five = inv_two * inv_two * inv
    quad_x = qxx * rx + qxy * ry + qxz * rz
    quad_y = qxy * rx + qyy * ry + qyz * rz
    quad_z = qxz * rx + qyz * ry + qzz * rz
    inner = rx * quad_x + ry * quad_y + rz * quad_z
    radial = 2.5 * inner * inv_two - mass * square
    total = lambda v: jnp.sum(v, axis=0, keepdims=True)
    return (
        total((radial * rx - quad_x) * inv_five),
        total((radial * ry - quad_y) * inv_five),
        total((radial * rz - quad_z) * inv_five),
    )


def kernel(
    n_sec,
    n_grp,
    pos_hbm,
    vel_hbm,
    mass_hbm,
    near_hbm,
    count_hbm,
    far_hbm,
    half_out,
    vel_out,
    direct_out,
    pos_ref,
    vel_ref,
    mass_ref,
    near_ref,
    count_ref,
    far_ref,
    ghosts,
    gathered,
    times,
    chosen,
    kept,
    spread,
    target_side,
    send_sem,
    recv_sem,
    moment_recv,
):
    n_dev = n_sec * n_grp
    local_blocks = near_ref.shape[0]
    slots = near_ref.shape[1]
    particles = pos_ref.shape[1]
    block_size = particles // local_blocks
    group_blocks = n_sec * local_blocks
    sec = lax.axis_index("sec")
    grp = lax.axis_index("grp")
    me = sec * n_grp + grp

    barrier = pltpu.get_barrier_semaphore()

    def take(load_sem):
        loads = [
            pltpu.make_async_copy(source, target, load_sem.at[k])
            for k, (source, target) in enumerate(
                (
                    (pos_hbm, pos_ref),
                    (vel_hbm, vel_ref),
                    (mass_hbm, mass_ref),
                    (near_hbm, near_ref),
                    (count_hbm, count_ref),
                    (far_hbm, far_ref),
                )
            )
        ]
        for load in loads:
            load.start()

        def greet(to_sec, to_grp):
            pl.semaphore_signal(
                barrier, inc=1, device_id={"sec": to_sec, "grp": to_grp}, device_id_type=MESH
            )

        each_other(n_sec, n_grp, sec, grp, greet)
        for load in loads:
            load.wait()

    pl.run_scoped(take, pltpu.SemaphoreType.DMA((6,)))

    number = lax.broadcasted_iota(jnp.int32, (group_blocks, slots), 0)
    slot = lax.broadcasted_iota(jnp.int32, (group_blocks, slots), 1)
    for b in range(local_blocks):
        used = jnp.where(
            (near_ref[b : b + 1, :] == number) & (slot < count_ref[b]), 1.0, 0.0
        )
        times[b] = jnp.broadcast_to(
            jnp.sum(used, axis=1, keepdims=True), (group_blocks, LANES)
        )
    entries = far_ref.shape[1]
    width = LANES // local_blocks
    half_of_lane = lax.broadcasted_iota(jnp.int32, (entries, LANES), 1) // width
    number = lax.broadcasted_iota(jnp.int32, (n_dev, entries), 0)
    for b in range(local_blocks):
        rows = slice(b * entries, (b + 1) * entries)
        picked = far_ref[b : b + 1, :]
        chosen[rows, :] = jnp.transpose(jnp.where(picked // local_blocks == number, 1.0, 0.0))
        place = jnp.transpose(
            jnp.broadcast_to((picked % local_blocks).astype(jnp.float32), (LANES, entries))
        )
        kept[rows, :] = jnp.where(place == half_of_lane.astype(jnp.float32), 1.0, 0.0)

    middles = None
    current = pos_ref[...]
    speed = vel_ref[...]

    source_lane = lax.broadcasted_iota(jnp.int32, (LANES, LANES), 0)
    for k in range(NUMBERS):
        spread[:, k * LANES : (k + 1) * LANES] = jnp.where(
            (source_lane % PLACES == k) & (source_lane % width < 3 * PLACES), 1.0, 0.0
        ).astype(jnp.bfloat16)
    tiles = particles // LANES
    tiles_of_block = block_size // LANES
    for step in range(2):
        half = current + 0.5 * timestep * speed
        ghosts[step, sec, 0:3, :] = half
        ghosts[step, sec, 3:4, :] = mass_ref[...]

        blocks = []
        for b in range(local_blocks):
            cut = slice(b * block_size, (b + 1) * block_size)
            blocks.append(
                (half[0:1, cut], half[1:2, cut], half[2:3, cut], mass_ref[0:1, cut])
            )
        gathered[step, me], middles = own_moments(blocks, middles)
        origin = [sum(c) / local_blocks for c in zip(*middles)]
        if step == 0:
            pl.semaphore_wait(barrier, n_dev - 1)
        mine = gathered.at[step, me]

        def send_moments(to_sec, to_grp):
            pltpu.make_async_remote_copy(
                src_ref=mine,
                dst_ref=mine,
                send_sem=send_sem.at[1],
                recv_sem=moment_recv.at[step],
                device_id={"sec": to_sec, "grp": to_grp},
                device_id_type=MESH,
            ).start()

        each_other(n_sec, n_grp, sec, grp, send_moments)

        for r in range(1, n_sec):
            other = lax.rem(sec + r, n_sec)
            pltpu.make_async_remote_copy(
                src_ref=ghosts.at[step, sec],
                dst_ref=ghosts.at[step, sec],
                send_sem=send_sem.at[0],
                recv_sem=recv_sem.at[step, r - 1],
                device_id={"sec": other, "grp": grp},
                device_id_type=MESH,
            ).start()

        line = lax.broadcasted_iota(jnp.int32, (ROWS, 1), 0)
        shift = jnp.where(
            line == 0, origin[0], jnp.where(line == 1, origin[1], jnp.where(line == 2, origin[2], 0.0))
        )

        @pl.when(sec >= 0)
        def _():
            near = [half[c : c + 1, :] - origin[c] for c in range(3)]
            reach = near[0] * near[0] + near[1] * near[1] + near[2] * near[2]
            target_side[...] = paired(
                three_parts(
                    jnp.concatenate(
                        [-2.0 * near[0], -2.0 * near[1], -2.0 * near[2], jnp.ones_like(reach), reach]
                        + [jnp.zeros_like(reach)] * 3,
                        axis=0,
                    )
                ),
                TARGET_ORDER,
            )

        def add_device(r, totals):
            other = peer(sec, r, n_sec)

            @pl.when(r > 0)
            def _():
                pltpu.make_async_copy(
                    ghosts.at[step, other],
                    ghosts.at[step, other],
                    recv_sem.at[step, lax.rem(sec - other + n_sec, n_sec) - 1],
                ).wait()

            totals = [list(t) for t in totals]
            for tile in range(tiles):
                rows = ghosts[step, other, :, tile * LANES : (tile + 1) * LANES]
                rows = jnp.concatenate([rows, jnp.zeros_like(rows)], axis=0) - shift
                moved = jnp.where(line < 3, rows, 0.0)
                reach = jnp.sum(moved * moved, axis=0, keepdims=True) + softening
                source_side = three_parts(
                    jnp.where(line == 3, reach, jnp.where(line == 4, 1.0, moved))
                )
                square = lax.dot_general(
                    paired(source_side, SOURCE_ORDER),
                    target_side[...],
                    (((0,), (0,)), ((), ())),
                    preferred_element_type=jnp.float32,
                )
                columns = jnp.transpose(rows)
                place = tile // tiles_of_block
                weights = [
                    times[b, pl.ds(other * local_blocks + place, 1), :]
                    for b in range(local_blocks)
                ]
                for part in range(LANES // ROWS):
                    cut = slice(part * ROWS, (part + 1) * ROWS)
                    sx, sy, sz, sm = (
                        jnp.broadcast_to(columns[cut, c : c + 1], (ROWS, LANES)) for c in range(4)
                    )
                    scaled = [sm * w for w in weights]
                    for t in range(tiles):
                        inv = lax.rsqrt(square[cut, t * LANES : (t + 1) * LANES])
                        weight = scaled[t // tiles_of_block] * inv * (inv * inv)
                        totals[t][0] = totals[t][0] + weight * sx
                        totals[t][1] = totals[t][1] + weight * sy
                        totals[t][2] = totals[t][2] + weight * sz
                        totals[t][3] = totals[t][3] + weight
            return tuple(tuple(t) for t in totals)

        zero = jnp.zeros((ROWS, LANES), jnp.float32)
        totals = lax.fori_loop(0, n_sec, add_device, tuple((zero,) * 4 for _ in range(tiles)))
        summed = [
            jnp.concatenate(
                [jnp.sum(totals[t][c], axis=0, keepdims=True) for t in range(tiles)], axis=1
            )
            for c in range(4)
        ]
        direct = jnp.concatenate(
            [summed[c] - (half[c : c + 1, :] - origin[c]) * summed[3] for c in range(3)], axis=0
        )

        others = gathered.at[step, pl.ds(0, n_dev - 1)]
        sent = ghosts.at[step, pl.ds(0, n_sec - 1)]
        pltpu.make_async_copy(sent, sent, send_sem.at[0]).wait()
        pltpu.make_async_copy(others, others, send_sem.at[1]).wait()
        pltpu.make_async_copy(others, others, moment_recv.at[step]).wait()
        table = gathered[step].reshape(n_dev, LANES)
        parts = jnp.dot(
            chosen[...].astype(jnp.bfloat16),
            table.astype(jnp.bfloat16),
            preferred_element_type=jnp.float32,
        )
        numbers = jnp.dot(
            (parts * kept[...]).astype(jnp.bfloat16), spread[...], preferred_element_type=jnp.float32
        )
        far = []
        for b in range(local_blocks):
            moment = [
                jnp.concatenate(
                    [numbers[b * entries : (b + 1) * entries, k * LANES : (k + 1) * LANES]]
                    * tiles_of_block,
                    axis=1,
                )
                for k in range(NUMBERS)
            ]
            cut = slice(b * block_size, (b + 1) * block_size)
            far.append(
                jnp.concatenate(
                    far_part((half[0:1, cut], half[1:2, cut], half[2:3, cut]), moment), axis=0
                )
            )
        far = jnp.concatenate(far, axis=1)
        if step == 0:
            speed = speed + timestep * (direct + far)
            current = half + 0.5 * timestep * speed
            vel_out[...] = speed
        else:
            half_out[...] = half
            direct_out[...] = 0.5 * (direct + far)


def on_device(n_sec, n_grp, positions, velocities, masses, near_list, near_count, far_list):
    particles = positions.shape[1]
    local_blocks = near_list.shape[0]
    vmem = pl.BlockSpec(memory_space=pltpu.VMEM)
    half, speed, halved = pl.pallas_call(
        functools.partial(kernel, n_sec, n_grp),
        out_shape=[jax.ShapeDtypeStruct(positions.shape, jnp.float32)] * 3,
        in_specs=[pl.BlockSpec(memory_space=pltpu.HBM)] * 6,
        out_specs=[vmem] * 3,
        scratch_shapes=[
            pltpu.VMEM(positions.shape, jnp.float32),
            pltpu.VMEM(velocities.shape, jnp.float32),
            pltpu.VMEM((1, particles), jnp.float32),
            pltpu.VMEM(near_list.shape, jnp.int32),
            pltpu.SMEM(near_count.shape, jnp.int32),
            pltpu.VMEM(far_list.shape, jnp.int32),
            pltpu.VMEM((2, n_sec, 4, particles), jnp.float32),
            pltpu.VMEM((2, n_sec * n_grp, 1, LANES), jnp.float32),
            pltpu.VMEM((local_blocks, n_sec * local_blocks, LANES), jnp.float32),
            pltpu.VMEM(
                (local_blocks * far_list.shape[1], n_sec * n_grp), jnp.float32
            ),
            pltpu.VMEM((local_blocks * far_list.shape[1], LANES), jnp.float32),
            pltpu.VMEM((LANES, NUMBERS * LANES), jnp.bfloat16),
            pltpu.VMEM((len(TARGET_ORDER) * ROWS, particles), jnp.bfloat16),
            pltpu.SemaphoreType.DMA((2,)),
            pltpu.SemaphoreType.DMA((2, n_sec - 1)),
            pltpu.SemaphoreType.DMA((2,)),
        ],
        compiler_params=pltpu.CompilerParams(
            collective_id=0, has_side_effects=True, vmem_limit_bytes=16 * 1024 * 1024
        ),
        name="leapfrog",
    )(*[pltpu.with_memory_space_constraint(v, pltpu.HBM) for v in (positions, velocities, masses[None, :], near_list, near_count, far_list)])
    accel = halved + halved
    speed = speed + timestep * accel
    return half + 0.5 * timestep * speed, speed, accel


def solution(mesh):
    placed = (
        P(None, ("sec", "grp")),
        P(None, ("sec", "grp")),
        P(("sec", "grp")),
        P(("sec", "grp"), None),
        P(("sec", "grp")),
        P(("sec", "grp"), None),
    )
    return jax.shard_map(
        functools.partial(on_device, mesh.shape["sec"], mesh.shape["grp"]),
        mesh=mesh,
        in_specs=placed,
        out_specs=(P(None, ("sec", "grp")), P(None, ("sec", "grp")), P(None, ("sec", "grp"))),
        check_vma=False,
    )
```
